32 devices in a mesh: rep: 1, dp: 32 (over x, y, z, core).
Axes of the slice: x: 2, y: 2, z: 4, core: 2. Of those that a mesh axis runs over, the one named last changes fastest.
Arguments:
- x: bfloat16 [32, 2048, 640], P(('rep', 'dp'))
- dy: bfloat16 [32, 2048, 640], P(('rep', 'dp'))
- wq: bfloat16 [2, 640, 1024], P(None, 'dp')
- wk: bfloat16 [2, 640, 128], P(None, 'dp')
- wv: bfloat16 [2, 640, 128], P(None, 'dp')
- wo: bfloat16 [2, 1024, 640], P(None, 'dp')
- w_gate: bfloat16 [2, 640, 3200], P(None, 'dp')
- w_up: bfloat16 [2, 640, 3200], P(None, 'dp')
- w_down: bfloat16 [2, 3200, 640], P(None, 'dp')
Outputs:
- output 1: bfloat16 [32, 2048, 640], P(('rep', 'dp'))
- output 2: bfloat16 [2, 640, 1024], P('rep', 'dp')
- output 3: bfloat16 [2, 640, 128], P('rep', 'dp')
- output 4: bfloat16 [2, 640, 128], P('rep', 'dp')
- output 5: bfloat16 [2, 1024, 640], P('rep', 'dp')
- output 6: bfloat16 [2, 640, 3200], P('rep', 'dp')
- output 7: bfloat16 [2, 640, 3200], P('rep', 'dp')
- output 8: bfloat16 [2, 3200, 640], P('rep', 'dp')
All inputs are finite; a program needn't handle non-finite values.
Results may differ from the reference program's by a relative error of at most 0.0273.
Values are sent between devices in bfloat16 or wider.
A program may use at most 2 GiB of HBM per device.

```python
import jax
import jax.numpy as jnp
from jax import lax

SEQUENCES = 32
TOKENS = 2048
D = 640
HEADS = 8
KV_HEADS = 1
HEAD = 128
FF = 3200
LAYERS = 2
THETA = 10000
NAMES = ("wq", "wk", "wv", "wo", "w_gate", "w_up", "w_down")
SHAPES = {
    "wq": (LAYERS, D, HEADS * HEAD),
    "wk": (LAYERS, D, KV_HEADS * HEAD),
    "wv": (LAYERS, D, KV_HEADS * HEAD),
    "wo": (LAYERS, HEADS * HEAD, D),
    "w_gate": (LAYERS, D, FF),
    "w_up": (LAYERS, D, FF),
    "w_down": (LAYERS, FF, D),
}


def bump(key, n, height):
    away = (jnp.arange(n, dtype=jnp.int32) - jax.random.randint(key, (), 0, n, jnp.int32)) % n
    return jnp.where(away < n // 8, height, 1.0)


def together(key, own, strength):
    shared = jax.random.normal(key, own.shape[1:], jnp.float32)
    return (own + strength * shared) * lax.rsqrt(1 + strength * strength)


def setup_inputs(seed: int = 0, part: int = 0) -> dict:
    kx, kdy, ka, kb, kz, kf, kh, kl, *keys = jax.random.split(jax.random.key(seed), 8 + 3 * len(NAMES))
    kx, kdy, ka, kb = (jax.random.fold_in(k, part) for k in (kx, kdy, ka, kb))
    kw, km, kv = (keys[i::3] for i in range(3))
    shape = (SEQUENCES, TOKENS, D)
    much_x, much_dy = jax.random.uniform(kz, (2,), jnp.float32, 0.0, 1.0)
    loud = 2.0 ** jax.random.uniform(jax.random.fold_in(kz, 1), (), jnp.float32, -1.0, 2.0)
    layers = 2.0 ** jax.random.uniform(kl, (LAYERS, 1, 1), jnp.float32, -1.0, 1.0)
    times = {"wq": 1.0, "wk": 1.0, "wv": 2.0, "wo": layers, "w_gate": 1.0, "w_up": bump(kh, FF, 4.0), "w_down": layers}
    x = together(ka, jax.random.normal(kx, shape, jnp.float32), much_x) * bump(kf, D, 4.0)
    dy = together(kb, jax.random.normal(kdy, shape, jnp.float32), much_dy)
    drawn = {"x": x.astype(jnp.bfloat16), "dy": (loud * dy * (SEQUENCES * TOKENS) ** -0.5).astype(jnp.bfloat16)}
    for key, name in zip(kw, NAMES, strict=True):
        drawn[name] = (jax.random.normal(key, SHAPES[name], jnp.float32) * SHAPES[name][1] ** -0.5 * times[name]).astype(jnp.bfloat16)
    return drawn


def matmul(a, w):
    return jnp.dot(a, w, preferred_element_type=jnp.float32).astype(jnp.bfloat16)


def normed(h):
    wide = h.astype(jnp.float32)
    scale = lax.rsqrt(jnp.mean(wide**2, -1, keepdims=True) + 1e-6)
    return (wide * scale).astype(jnp.bfloat16)


def turned(t, theta):
    half = t.shape[-1] // 2
    angle = jnp.arange(t.shape[0], dtype=jnp.float32)[:, None] * theta ** (-jnp.arange(half, dtype=jnp.float32) / half)
    cos, sin = jnp.cos(angle)[:, None], jnp.sin(angle)[:, None]
    a, b = t[..., :half].astype(jnp.float32), t[..., half:].astype(jnp.float32)
    return jnp.concatenate([a * cos - b * sin, b * cos + a * sin], -1).astype(jnp.bfloat16)


def seen_by(q, k, v):
    tokens, kv = q.shape[0], k.shape[1]
    q = q.reshape(tokens, kv, -1, q.shape[-1])
    scores = jnp.einsum("tgsd,ugd->gstu", q.astype(jnp.float32), k.astype(jnp.float32)) * q.shape[-1] ** -0.5
    place = jnp.arange(tokens)
    weights = jax.nn.softmax(jnp.where(place[:, None] >= place, scores, -jnp.inf), -1).astype(jnp.bfloat16)
    return jnp.einsum("gstu,ugd->tgsd", weights.astype(jnp.float32), v.astype(jnp.float32)).astype(jnp.bfloat16).reshape(tokens, -1)


def layer(h, w):
    a = normed(h)
    q, k = (turned(matmul(a, w[name]).reshape(h.shape[0], -1, HEAD), THETA) for name in ("wq", "wk"))
    h = h + matmul(seen_by(q, k, matmul(a, w["wv"]).reshape(h.shape[0], -1, HEAD)), w["wo"])
    b = normed(h)
    gate = jnp.dot(b, w["w_gate"], preferred_element_type=jnp.float32)
    up = jnp.dot(b, w["w_up"], preferred_element_type=jnp.float32)
    return h + matmul((jax.nn.silu(gate) * up).astype(jnp.bfloat16), w["w_down"])


def stack(weights, h):
    return lax.scan(lambda h, w: (layer(h, w), None), h, weights)[0]


def reference(x, dy, wq, wk, wv, wo, w_gate, w_up, w_down):
    weights = dict(zip(NAMES, (wq, wk, wv, wo, w_gate, w_up, w_down), strict=True))

    def take(so_far, sequence):
        h, by_y = sequence
        _, back = jax.vjp(stack, weights, h)
        by_weights, by_h = back(by_y)
        return jax.tree.map(lambda total, term: total + term.astype(jnp.float32), so_far, by_weights), by_h

    none_yet = {name: jnp.zeros(w.shape, jnp.float32) for name, w in weights.items()}
    by_weights, by_x = lax.scan(take, none_yet, (x, dy))
    return (by_x, *(by_weights[name].astype(jnp.bfloat16) for name in NAMES))
```

```python
import collections

import jax
import jax.numpy as jnp
import numpy as np
from jax import lax
from jax.experimental import pallas as pl
from jax.experimental.pallas import tpu as pltpu
from jax.sharding import PartitionSpec as P


def ints(text):
    return tuple(map(int, text.split(",")))


D, HEADS, HEAD, FF, TOKENS, THETA = ints("640,8,128,3200,2048,10000")
FFS = tuple(map(ints, ("0,1280", "1280,1280", "2560,640")))
BK = 512
SCALE, LOG2E, HIDDEN = HEAD**-0.5, 1.4426950408889634, -2e30
F32, BF16 = jnp.float32, jnp.bfloat16
CORES = HERE, THERE = (0, 1)
VMEM_MAX = 63 * 2**20
STOPS = 1


def dot(a, b, ca=1, cb=0):
    return lax.dot_general(a, b, (((ca,), (cb,)), ((), ())), preferred_element_type=F32)


def dot_t(a, b):
    return dot(a, b, 1, 1)


def rope_tables():
    half = HEAD // 2
    rate = np.float32(THETA) ** (-np.arange(half, dtype=np.float32) / np.float32(half))
    angle = (np.arange(TOKENS, dtype=np.float32)[:, None] * rate).astype(np.float64)
    cos, sin = np.cos(angle), np.sin(angle)
    return np.concatenate([cos, cos], 1).astype(np.float32), np.concatenate([-sin, sin], 1).astype(np.float32)


def norm(h):
    wide = h.astype(F32)
    scale = lax.rsqrt(jnp.mean(wide * wide, -1, keepdims=True) + 1e-6)
    return wide, scale, (wide * scale).astype(BF16)


def norm_back(wide, scale, by):
    return (scale * by - wide * (scale * scale * scale * jnp.mean(by * wide, -1, keepdims=True))).astype(BF16)


def turn(t, cos, sin):
    return t * cos + pltpu.roll(t, HEAD // 2, 1) * sin


def turn_back(t, cos, sin):
    return t * cos + pltpu.roll(t * sin, HEAD // 2, 1)


def whole(*shape):
    return pl.BlockSpec(shape, lambda *_: (0,) * len(shape), pipeline_mode=pl.Buffered(1))


def rows(t, n=D):
    return pl.BlockSpec((t, n), lambda i: (i, 0))


def heads(t, at=lambda i: i):
    return pl.BlockSpec((HEADS, t, HEAD), lambda i: (0, at(i), 0))


def stats(t, at=lambda i: i):
    return pl.BlockSpec((HEADS, t), lambda i: (0, at(i)))


def like(*shape, t=BF16):
    return jax.ShapeDtypeStruct(shape, t)


def nothing(*_):
    pass


def call(body, grid, ins, outs, scratch=(), link=(), stops=1, flops=0, exps=0):
    job = link[0] if link else ()
    xins, xouts, xscratch = (job.ins, job.outs, job.scratch) if link else ((), (), ())
    sizes = [len(ins), len(xins), len(outs), len(xouts), len(scratch), len(xscratch)]

    def kernel(*refs):
        groups = []
        for n in sizes:
            groups.append(refs[:n])
            refs = refs[n:]
        ours, more = [sum(groups[i::2], ()) for i in CORES]
        step = pl.program_id(0)
        if link:
            job.begin(step, more, grid, stops)
        body(step, job.stop if link else nothing, *ours)
        if link:
            job.finish()

    ins, outs = [*ins, *xins], [*outs, *xouts]
    params = dict(collective_id=link[1], has_side_effects=True) if link else {}
    moved = sum(a.size * a.dtype.itemsize for a in (*[i[0] for i in ins], *[o[0] for o in outs]))
    got = pl.pallas_call(
        kernel,
        grid=(grid,),
        in_specs=[i[1] for i in ins],
        out_specs=[o[1] for o in outs],
        out_shape=[o[0] for o in outs],
        scratch_shapes=[*scratch, *xscratch],
        compiler_params=pltpu.CompilerParams(dimension_semantics=("arbitrary",), vmem_limit_bytes=VMEM_MAX, **params),
        cost_estimate=pl.CostEstimate(flops=flops, transcendentals=exps, bytes_accessed=moved),
    )(*[i[0] for i in ins])
    n = sizes[2]
    return (got[:n], job.results(got[n:])) if link else got


def qkv(h, w, cos, sin, link=(), t=512):
    def body(_, stop, h_ref, wq_ref, wkv_ref, cos_ref, sin_ref, q_ref, k_ref, v_ref):
        _, _, a = norm(h_ref[...])
        cos, sin = cos_ref[...], sin_ref[...]
        q = dot(a, wq_ref[...]).astype(BF16).astype(F32)
        for n in range(HEADS):
            q_ref[n] = turn(q[:, n * HEAD : (n + 1) * HEAD], cos, sin).astype(BF16)
        k_ref[...] = turn(dot(a, wkv_ref[0]).astype(BF16).astype(F32), cos, sin).astype(BF16)
        v_ref[...] = dot(a, wkv_ref[1]).astype(BF16)

    ins = [(h, rows(t)), (w["q"], whole(D, HEADS * HEAD)), (w["kv"], whole(2, D, HEAD)), (cos, rows(t, HEAD)), (sin, rows(t, HEAD))]
    outs = [(like(HEADS, TOKENS, HEAD), heads(t))] + [(like(TOKENS, HEAD), rows(t, HEAD))] * 2
    return call(body, TOKENS // t, ins, outs, link=link, flops=2 * TOKENS * D * (HEADS + 2) * HEAD)


def joined(o_ref):
    return jnp.concatenate([o_ref[n] for n in range(HEADS)], axis=1)


def weights_of(w):
    return [(w["o"], whole(HEADS * HEAD, D)), (w["gu"], whole(2, D, FF)), (w["d"], whole(FF, D))]


def after(o, h, w, link=(), t=256):
    def body(_, stop, o_ref, h_ref, wo_ref, wgu_ref, wd_ref, mid_ref, out_ref):
        mid = h_ref[...] + dot(joined(o_ref), wo_ref[...]).astype(BF16)
        mid_ref[...] = mid
        _, _, b = norm(mid)
        total = 0.0
        for at, n in FFS:
            stop()
            part = pl.ds(at, n)
            gate, up = (dot(b, wgu_ref[i, :, part]) for i in CORES)
            total += dot((gate * jax.nn.sigmoid(gate) * up).astype(BF16), wd_ref[part, :])
        out_ref[...] = mid + total.astype(BF16)

    ins = [(o, heads(t)), (h, rows(t)), *weights_of(w)]
    return call(body, TOKENS // t, ins, [(like(TOKENS, D), rows(t))] * 2, link=link, stops=4, flops=2 * TOKENS * D * (HEADS * HEAD + 3 * FF))


def after_back(by, mid, o, w, link=(), t=256):
    grid = TOKENS // t
    pieces, most = FF // D, D

    def body(step, stop, by_ref, mid_ref, o_ref, wo_ref, wgu_ref, wd_ref, bymid_ref, byo_ref, delta_ref, gu_hbm, d_hbm, o_hbm,
             acc_gu, acc_d, acc_o, st_gu, st_d, st_o, sem_gu, sem_d, sem_o):
        first, last = step == 0, step == grid - 1
        by = by_ref[...]
        wide, scale, b = norm(mid_ref[...])
        bt, byt = b.T, by.T

        def add(ref, v):
            ref[...] = jnp.where(first, 0.0, ref[...]) + v

        def leaving(i):
            at = pl.ds(i * most, most)
            return [pltpu.make_async_copy(st_gu.at[i % 2], gu_hbm.at[:, :, at], sem_gu.at[i % 2]),
                    pltpu.make_async_copy(st_d.at[i % 2], d_hbm.at[at, :], sem_d.at[i % 2])]

        byb = 0.0
        for at, n in FFS:
            stop()
            part = pl.ds(at, n)
            gate, up = (dot(b, wgu_ref[i, :, part]) for i in CORES)
            byp = dot_t(by, wd_ref[part, :]).astype(BF16).astype(F32)
            s = jax.nn.sigmoid(gate)
            silu = gate * s
            add(acc_d.at[:, part], dot(byt, (silu * up).astype(BF16)))
            bys = (byp * up * (s + silu * (1.0 - s))).astype(BF16), (byp * silu).astype(BF16)
            for i in CORES:
                add(acc_gu.at[i, :, part], dot(bt, bys[i]))
                byb += dot_t(bys[i], wgu_ref[i, :, part])

            @pl.when(last)
            def _():
                for i in range(at // most, (at + n) // most):
                    piece = pl.ds(i * most, most)
                    if i > 1:
                        for c in leaving(i - 2):
                            c.wait()
                    st_gu[i % 2] = acc_gu[:, :, piece].astype(BF16)
                    st_d[i % 2] = acc_d[:, piece].T.astype(BF16)
                    for c in leaving(i):
                        c.start()

        bymid = by + norm_back(wide, scale, byb.astype(BF16).astype(F32))
        bymid_ref[...] = bymid
        byo = dot_t(bymid, wo_ref[...]).astype(BF16)
        o = joined(o_ref)
        add(acc_o, dot(o.T, bymid))
        for n in range(HEADS):
            one = slice(n * HEAD, (n + 1) * HEAD)
            byo_ref[n] = byo[:, one]
            delta_ref[n : n + 1, :] = (byo[:, one].astype(F32) * o[:, one].astype(F32)).T.sum(0, keepdims=True)

        @pl.when(last)
        def _():
            st_o[...] = acc_o[...].astype(BF16)
            c = pltpu.make_async_copy(st_o, o_hbm, sem_o)
            c.start()
            for x in (*leaving(pieces - 2), *leaving(pieces - 1), c):
                x.wait()

    ins = [(by, rows(t)), (mid, rows(t)), (o, heads(t)), *weights_of(w)]
    outs = [(like(TOKENS, D), rows(t)), (like(HEADS, TOKENS, HEAD), heads(t)), (like(HEADS, TOKENS, t=F32), stats(t)),
            (like(2, D, FF), HBM), (like(FF, D), HBM), (like(HEADS * HEAD, D), HBM)]
    scratch = [regs((2, D, FF), F32), regs((D, FF), F32), regs((HEADS * HEAD, D), F32), regs((2, 2, D, most), BF16), regs((2, most, D), BF16),
               regs((HEADS * HEAD, D), BF16), dma((2,)), dma((2,)), dma]
    return call(body, grid, ins, outs, scratch, link, 4, flops=2 * TOKENS * D * (2 * HEADS * HEAD + 8 * FF))


def qkv_back(dq, dk, dv, h, bymid, w, cos, sin, link=(), t=512):
    grid = TOKENS // t

    def body(step, stop, dq_ref, dk_ref, dv_ref, h_ref, bymid_ref, wq_ref, wkv_ref, cos_ref, sin_ref, byh_ref, gq_ref, gkv_ref, acc_q, acc_kv):
        first, last = step == 0, step == grid - 1
        cos, sin = cos_ref[...], sin_ref[...]
        wide, scale, a = norm(h_ref[...])
        at = a.T
        dq = jnp.concatenate([turn_back(dq_ref[n].astype(F32), cos, sin).astype(BF16) for n in range(HEADS)], axis=1)
        dkv = turn_back(dk_ref[...].astype(F32), cos, sin).astype(BF16), dv_ref[...]
        acc_q[...] = jnp.where(first, 0.0, acc_q[...]) + dot(at, dq)
        bya = dot_t(dq, wq_ref[...])
        for i in CORES:
            acc_kv[i] = jnp.where(first, 0.0, acc_kv[i]) + dot(at, dkv[i])
            bya += dot_t(dkv[i], wkv_ref[i])
        byh_ref[...] = bymid_ref[...] + norm_back(wide, scale, bya.astype(BF16).astype(F32))

        @pl.when(last)
        def _():
            gq_ref[...] = acc_q[...].astype(BF16)
            gkv_ref[...] = acc_kv[...].astype(BF16)

    wq, wkv = whole(D, HEADS * HEAD), whole(2, D, HEAD)
    ins = [(dq, heads(t)), (dk, rows(t, HEAD)), (dv, rows(t, HEAD)), (h, rows(t)), (bymid, rows(t)), (w["q"], wq), (w["kv"], wkv), (cos, rows(t, HEAD)), (sin, rows(t, HEAD))]
    outs = [(like(TOKENS, D), rows(t)), (like(D, HEADS * HEAD), wq), (like(2, D, HEAD), wkv)]
    scratch = [regs((D, HEADS * HEAD), F32), regs((2, D, HEAD), F32)]
    return call(body, grid, ins, outs, scratch, link, flops=4 * TOKENS * D * (HEADS + 2) * HEAD)


def fwd_place(s):
    iq = sum(jnp.minimum(s // n, 1) for n in ints("1,3,6"))
    return iq, s - iq * (iq + 1) // 2


def attend(q, k, v, link=()):
    blocks, e = 10, SCALE * LOG2E
    at = lambda s: fwd_place(s)[0]

    def body(s, stop, q_ref, k_ref, v_ref, o_ref, lse_ref, top_s, mix_s):
        iq, jk = fwd_place(s)
        keys = pl.ds(pl.multiple_of(jk * BK, BK), BK)

        @pl.when(jk == 0)
        def _():
            top_s[...] = jnp.full(top_s.shape, HIDDEN / 2, F32)
            mix_s[...] = jnp.zeros(mix_s.shape, F32)

        def block(masked, some):
            k = k_ref[keys, :]
            values = jnp.concatenate([v_ref[keys, :].T, jnp.ones((8, BK), BF16)], axis=0)
            scores = [dot_t(k, q_ref[n]) for n in some]
            weights, keeps = [], []
            for n, x in zip(some, scores):
                if masked:
                    x = jnp.where(lax.broadcasted_iota(jnp.int32, x.shape, 1) >= lax.broadcasted_iota(jnp.int32, x.shape, 0), x, HIDDEN)
                one = slice(n, n + 1)
                old = top_s[one, :]
                top = jnp.maximum(old, x.max(axis=0, keepdims=True))
                top_s[one, :] = top
                weights.append(jnp.exp2((x - top) * e).astype(BF16))
                keeps.append(jnp.exp2((old - top) * e))
            for n, p, keep in zip(some, weights, keeps):
                mix_s[n] = mix_s[n] * keep + dot(values, p)

        def last(some):
            block(True, some)
            for n in some:
                total = mix_s[n, HEAD : HEAD + 1, :]
                o_ref[n] = (mix_s[n, :HEAD, :] * (1.0 / total)).T.astype(BF16)
                lse_ref[n : n + 1, :] = top_s[n : n + 1, :] * SCALE + jnp.log(total)

        for at in range(0, HEADS, HEADS // STOPS):
            if at:
                stop()
            some = range(at, at + HEADS // STOPS)
            pl.when(jk < iq)(lambda: block(False, some))
            pl.when(jk == iq)(lambda: last(some))

    kv = whole(TOKENS, HEAD)
    return call(body, blocks, [(q, heads(BK, at)), (k, kv), (v, kv)],
                [(like(HEADS, TOKENS, HEAD), heads(BK, at)), (like(HEADS, TOKENS, t=F32), stats(BK, at))],
                [regs((HEADS, BK), F32), regs((HEADS, HEAD + 8, BK), F32)], link, STOPS,
                flops=4 * blocks * BK * BK * HEADS * HEAD, exps=blocks * BK * BK * HEADS)


def back_place(s):
    g = sum(jnp.minimum(s // n, 1) for n in ints("2,6,12"))
    r = s - g * (g + 1)
    second = jnp.minimum(r // (g + 1), 1)
    return g, 2 * g + second, r - second * (g + 1)


def attend_back(q, k, v, byo, lse, delta, link=()):
    blocks, e, bq = 20, SCALE * LOG2E, BK // 2
    at = lambda s: back_place(s)[1]
    pairs = range(0, HEADS, 2)

    def body(s, stop, q_ref, k_ref, v_ref, do_ref, lse_ref, delta_ref, dq_ref, dk_ref, dv_ref, dq_s, dk_s, dv_s):
        g, iq, jk = back_place(s)
        keys = pl.ds(pl.multiple_of(jk * BK, BK), BK)
        row = lambda ref, n: jnp.concatenate([ref[n : n + 1, :], ref[n + 1 : n + 2, :]], axis=1)

        @pl.when(s == 0)
        def _():
            dk_s[...] = jnp.zeros(dk_s.shape, F32)
            dv_s[...] = jnp.zeros(dv_s.shape, F32)

        @pl.when(jk == 0)
        def _():
            dq_s[...] = jnp.zeros(dq_s.shape, F32)

        def block(masked, some):
            k, v = k_ref[keys, :], v_ref[keys, :]
            kt = k.T
            qs = [q_ref[n : n + 2].reshape(2 * bq, HEAD) for n in some]
            dos = [do_ref[n : n + 2].reshape(2 * bq, HEAD) for n in some]
            scores = [dot_t(k, x) for x in qs]
            dps = [dot_t(v, x) for x in dos]
            for i, n in enumerate(some):
                p = jnp.exp2(scores[i] * e - row(lse_ref, n) * LOG2E)
                if masked:
                    ahead = lax.rem(lax.broadcasted_iota(jnp.int32, p.shape, 1), bq) - lax.broadcasted_iota(jnp.int32, p.shape, 0)
                    p = jnp.where(ahead >= jk * BK - iq * bq, p, 0.0)
                ds = (p * (dps[i] - row(delta_ref, n))).astype(BF16)
                dv_s[keys, :] += dot(p.astype(BF16), dos[i])
                dk_s[keys, :] += dot(ds, qs[i])
                dq_s[n // 2] += dot(kt, ds)

        def last(some):
            block(True, some)
            for n in some:
                dq_ref[n : n + 2] = (dq_s[n // 2] * SCALE).T.reshape(2, bq, HEAD).astype(BF16)

        for at in range(0, HEADS, HEADS // STOPS):
            if at:
                stop()
            some = pairs[at // 2 : (at + HEADS // STOPS) // 2]
            pl.when(jk < g)(lambda: block(False, some))
            pl.when(jk == g)(lambda: last(some))

        @pl.when(s == blocks - 1)
        def _():
            dk_ref[...] = (dk_s[...] * SCALE).astype(BF16)
            dv_ref[...] = dv_s[...].astype(BF16)

    kv = whole(TOKENS, HEAD)
    return call(body, blocks, [(q, heads(bq, at)), (k, kv), (v, kv), (byo, heads(bq, at)), (lse, stats(bq, at)), (delta, stats(bq, at))],
                [(like(HEADS, TOKENS, HEAD), heads(bq, at)), *[(like(TOKENS, HEAD), kv)] * 2],
                [regs((HEADS // 2, HEAD, BK), F32), regs((TOKENS, HEAD), F32), regs((TOKENS, HEAD), F32)], link, STOPS,
                flops=blocks * 5 * BK * BK * HEADS * HEAD, exps=blocks * BK * bq * HEADS)


def prep(weights):
    parts = [(name, lead) for name in ROWS for lead in ([(c,) for c in CORES] if LEAD[name] else [()])]
    names = list(ROWS)

    def kernel(*refs):
        refs = list(refs)
        own, blocks, here, there, sem = ([refs.pop(0) for _ in range(n)] for n in (len(parts), 2 * len(names), len(parts), len(parts), len(ZS)))
        p = Place()
        local = [pltpu.make_async_copy(a, b, sem[2].at[i]) for i, (a, b) in enumerate(zip(own, here))]
        for c in local:
            c.start()
        greet([p.partner])
        far = [send(a, b, sem, i, p.partner) for i, (a, b) in enumerate(zip(own, there))]
        for c in far:
            c.start()
        for i, (name, lead) in enumerate(parts):
            local[i].wait()
            far[i].wait()
            n = ROWS[name] // 2
            for core in CORES:

                @pl.when(p.core == core)
                def _():
                    for layer in CORES:
                        out = blocks[2 * names.index(name) + layer]
                        for at, src in ((core, here[i]), (1 - core, there[i])):
                            out[(*lead, pl.ds(at * n, n), ALL)] = src[layer]

    got = pl.pallas_call(
        kernel,
        in_specs=[HBM] * len(parts),
        out_specs=[VMEM] * 2 * len(names),
        out_shape=[like(*LEAD[n], ROWS[n], COLS[n]) for n in names for _ in CORES],
        scratch_shapes=[regs(w.shape, BF16) for w in weights] * 2 + [dma((len(parts),))] * len(ZS),
        compiler_params=pltpu.CompilerParams(collective_id=0, has_side_effects=True, vmem_limit_bytes=VMEM_MAX),
        name="prep",
    )(*weights)
    return {n: got[2 * i : 2 * i + 2] for i, n in enumerate(names)}


MESH = pl.DeviceIdType.MESH
ZS = ints("1,2,3")
NEAR = ints("1,3,2")
FAR = ints("2,1,3,0")
BLOCKS = ints("2,2,4")
ALL = slice(None)
HBM, VMEM = pl.BlockSpec(memory_space=pl.ANY), pl.BlockSpec(memory_space=pltpu.VMEM)
dma, regs = pltpu.SemaphoreType.DMA, pltpu.VMEM


class Place:
    def __init__(self):
        me = self.me = lax.axis_index("dp")
        chip = me // 2
        self.core, self.z, self.y, self.x = me % 2, chip % 4, chip // 4 % 2, chip // 8
        self.partner = me + 1 - 2 * self.core
        self.side = {"x": me + 16 * (1 - 2 * self.x), "y": me + 8 * (1 - 2 * self.y)}

    def zat(self, j):
        return (self.z + j + 4) % 4

    def zn(self, j):
        return self.me + 2 * (self.zat(j) - self.z)

    def at(self, order, f, s, j):
        own = dict(x=self.x, y=self.y)
        for a, other in zip(order, (f, s)):
            own[a] = 1 - own[a] if other else own[a]
        return own["x"], own["y"], self.zat(j)


def greet(peers):
    barrier = pltpu.get_barrier_semaphore()
    for p in peers:
        pl.semaphore_signal(barrier, inc=1, device_id=(0, p), device_id_type=MESH)
    pl.semaphore_wait(barrier, len(peers))


def everyone(p):
    return [p.partner, *p.side.values()] + [p.zn(j) for j in ZS]


def send(src, dst, sem, i, to):
    return pltpu.make_async_remote_copy(src_ref=src, dst_ref=dst, send_sem=sem[0].at[i], recv_sem=sem[1].at[i], device_id=(0, to), device_id_type=MESH)


ROWS = {k: n // 16 for k, n in dict(q=D, kv=D, o=HEADS * HEAD, gu=D, d=FF).items()}
COLS = dict(q=HEADS * HEAD, kv=HEAD, gu=FF, o=D, d=D)
LEAD = dict(q=(), kv=(2,), gu=(2,), o=(), d=())
ORDERS = ("yx", "xy")
GU_CUT = ints("0,1664"), ints("1664,1536")
O_CUT = ints("0,256"), ints("256,384")
D_CUT = ints("0,104"), ints("104,96")


Cut = collections.namedtuple("Cut", "lead,rows,cols,order,size,span")


def cuts(name, core):
    return [Cut(*c) for c in _cuts(name, core)]


def _cuts(name, core):
    if name == "q":
        half = COLS[name] // 4
        return [((), ALL, pl.ds(pl.multiple_of(core * 2 * half + i * half, half), half), o, (ROWS[name], half), (i * half, half)) for i, o in enumerate(ORDERS)]
    if name == "kv":
        return [((core,), ALL, ALL, ORDERS[0], (ROWS[name], HEAD), (0, HEAD))]
    if name == "gu":
        return [((core,), ALL, pl.ds(*c), o, (ROWS[name], c[1]), c) for c, o in zip(GU_CUT, ORDERS)]
    if name == "o":
        half = ROWS[name] // 2
        return [((), pl.ds(pl.multiple_of(core * half, half), half), pl.ds(*c), o, (half, c[1]), c) for c, o in zip(O_CUT, ORDERS)]
    return [((), pl.ds(*D_CUT[core]), ALL, ORDERS[core], (D_CUT[core][1], D), (0, D))]


def full_shape(name):
    return (*LEAD[name], *BLOCKS, ROWS[name], COLS[name])


def deal(p, names, make):
    units, low, n = [], ([], []), 0
    for name in names:
        if name == "d":
            for c in CORES:
                low[c].append(make(n, name, 0, c))
            n += 1
        else:
            for i in range(len(cuts(name, 0))):
                units.append(make(n, name, i, p.core))
                n += 1
    return units, low


def count(names):
    return sum(len(cuts(name, 0)) for name in names)


def over(p, sets, step):
    units, low = sets
    for u in units:
        step(u)
    for c in CORES:
        if low[c]:

            @pl.when(p.core == c)
            def _():
                for u in low[c]:
                    step(u)


class Gather:
    FIRST, SECOND, PARTNER, SENDS = ints("3,7,15,31")

    def __init__(self, p, n, full, block, cut, far, sems):
        self.p, self.order, self.sem, self.lsem = p, cut.order, [s.at[n] for s in sems[:2]], sems[2].at[n]
        self.full = lambda place: full.at[(*cut.lead, *place, cut.rows, cut.cols)]
        self.theirs = lambda place: full.at[(*far.lead, *place, far.rows, far.cols)]
        self.far_order = far.order
        self.block = block.at[(*cut.lead, cut.rows, cut.cols)]

    def at(self, f, s, j):
        return self.full(self.p.at(self.order, f, s, -j))

    def src(self, f, s, j):
        return self.at(f, s, j) if f or s or j else self.block

    def to_z(self, j):
        return send(self.block, self.at(HERE, HERE, HERE), self.sem, j - 1, self.p.zn(j))

    def to_first(self, j):
        return send(self.src(HERE, HERE, j), self.at(HERE, HERE, j), self.sem, self.FIRST + j, self.p.side[self.order[0]])

    def to_second(self, f, j):
        return send(self.src(f, HERE, j), self.at(f, HERE, j), self.sem, self.SECOND + 4 * f + j, self.p.side[self.order[1]])

    def to_partner(self, s, f, j):
        return send(self.src(f, s, j), self.at(f, s, j), self.sem, self.PARTNER + 8 * s + 4 * f + j, self.p.partner)

    def local(self):
        return pltpu.make_async_copy(self.block, self.at(HERE, HERE, HERE), self.lsem)

    def got(self, i, ref):
        send(ref, ref, self.sem, i, self.p.partner).wait_recv()

    def start(self):
        for j in FAR[:-1]:
            self.to_z(j).start()
        self.to_first(HERE).start()
        self.to_second(HERE, HERE).start()
        self.to_partner(HERE, HERE, HERE).start()
        self.local().start()

    def from_z(self, j):
        self.got(j - 1, self.at(HERE, HERE, j))
        self.to_first(j).start()
        self.to_second(HERE, j).start()
        self.to_partner(HERE, HERE, j).start()

    def from_first(self, j):
        self.got(self.FIRST + j, self.at(THERE, HERE, j))
        self.to_second(THERE, j).start()
        self.to_partner(HERE, THERE, j).start()

    def from_second(self, f, j):
        self.got(self.SECOND + 4 * f + j, self.at(f, THERE, j))
        self.to_partner(THERE, f, j).start()

    def finish(self):
        for s in CORES:
            for f in CORES:
                for j in range(4):
                    self.got(self.PARTNER + 8 * s + 4 * f + j, self.theirs(self.p.at(self.far_order, f, s, -j)))
        self.local().wait()
        for j in ZS:
            self.to_z(j).wait_send()
        for j in range(4):
            self.to_first(j).wait_send()
            for f in CORES:
                self.to_second(f, j).wait_send()
                for s in CORES:
                    self.to_partner(s, f, j).wait_send()


def gather_steps(p, sets):
    does = [lambda u: u.start()]
    order = [("from_z", NEAR[0]), ("from_first", HERE)] + [("from_z", j) for j in NEAR[1:]]
    for j, k in zip(NEAR, (HERE, *NEAR)):
        order += [("from_first", j), ("from_second", HERE, k)]
    order += [("from_second", HERE, NEAR[2])] + [("from_second", THERE, j) for j in (HERE, *NEAR)] + [("finish",)]
    does += [lambda u, o=o: getattr(u, o[0])(*o[1:]) for o in order]
    return [lambda d=d: over(p, sets, d) for d in does]


def gather_sems(names):
    n = count(names)
    return [dma((n, Gather.SENDS)), dma((n, Gather.SENDS)), dma((n,))]


def gather_sets(p, names, full, block, sems):
    return deal(p, names, lambda n, name, i, c: Gather(p, n, full[name], block[name], cuts(name, c)[i], cuts(name, 1 - c)[i], sems))


class Job:
    def begin(self, step, refs, grid, stops):
        self.step, self.grid, self.stops, self.at = step, grid, stops, 0
        p = self.p = Place()
        self.prepare(p, refs)

        @pl.when(step == 0)
        def _():
            self.before()
            greet(everyone(p))
            self.start()

        self.stop()

    def stop(self):
        places = self.grid * self.stops
        first = places * self.wait[0] // self.wait[1]
        for place in range(self.at, places, self.stops):
            mine = [x for i, x in enumerate(self.steps) if first + i * (places - first) // len(self.steps) == place]
            if mine:

                @pl.when(self.step == place // self.stops)
                def _():
                    for x in mine:
                        x()

        self.at += 1

    def finish(self):
        pl.when(self.step == self.grid - 1)(self.end)

    def before(self):
        pass


class GatherJob(Job):
    wait = ints("3,10")

    def __init__(self, blocks):
        self.names = tuple(blocks)
        self.ins = [(b, VMEM) for b in blocks.values()]
        self.outs = [(jax.ShapeDtypeStruct(full_shape(n), BF16), HBM) for n in self.names]
        self.scratch = gather_sems(self.names)

    def prepare(self, p, refs):
        n = len(self.names)
        sets = gather_sets(p, self.names, dict(zip(self.names, refs[n : 2 * n])), dict(zip(self.names, refs[:n])), refs[2 * n :])
        self.start, *self.steps, self.end = gather_steps(p, sets)

    def results(self, outs):
        return {n: whole_matrix(n, o) for n, o in zip(self.names, outs)}


def whole_matrix(name, full):
    return full.reshape(*LEAD[name], -1, COLS[name])


class Scatter:
    FIRST, SECOND, Z, SENDS, LOADS = ints("16,20,24,27,16")

    def __init__(self, p, n, name, full, cut, far, bufs, far_part, sems):
        self.p, self.name, self.cols, self.n = p, name, cut.span, n
        self.order, self.far_order = cut.order[::-1], far.order[::-1]
        self.sem, self.lsem = [s.at[n] for s in sems[:2]], sems[2].at[n]
        self.term = lambda place: full.at[(*cut.lead, *place, cut.rows, cut.cols)]
        self.given = lambda place: full.at[(*far.lead, *place, far.rows, far.cols)]
        self.own, self.part, self.r1, self.r2, self.r3, self.fin = bufs
        self.far_part = far_part

    def load(self, j, f, s):
        return pltpu.make_async_copy(self.term(self.p.at(self.order, f, s, j)), self.own.at[j, f, s], self.lsem.at[4 * j + 2 * f + s])

    def give(self, j, f, s):
        return send(self.given(self.p.at(self.far_order, f, s, j)), self.far_part.at[j, f, s], self.sem, 4 * j + 2 * f + s, self.p.partner)

    def hop1(self, j):
        return send(self.own.at[j, THERE], self.r1.at[j], self.sem, self.FIRST + j, self.p.side[self.order[0]])

    def hop2(self, j):
        return send(self.own.at[j, HERE, THERE], self.r2.at[j], self.sem, self.SECOND + j, self.p.side[self.order[1]])

    def hop3(self, j):
        return send(self.own.at[j, HERE, HERE], self.r3.at[j - 1], self.sem, self.Z + j - 1, self.p.zn(j))

    def begin(self, j, what):
        for f in (1, 0):
            for s in (1, 0):
                what(j, f, s).start()

    def two(self, j, f, s):
        self.load(j, f, s).wait()
        here = self.part.at[j, f, s]
        send(here, here, self.sem, 4 * j + 2 * f + s, self.p.partner).wait_recv()
        return self.own[j, f, s].astype(F32) + self.part[j, f, s].astype(F32)

    def step1(self, j):
        for s in CORES:
            self.own[j, THERE, s] = self.two(j, THERE, s).astype(BF16)
        self.hop1(j).start()

    def step2(self, j):
        self.hop1(j).wait_recv()
        self.own[j, HERE, THERE] = (self.two(j, HERE, THERE) + self.r1[j, 1].astype(F32)).astype(BF16)
        self.hop2(j).start()

    def step3(self, j):
        self.hop2(j).wait_recv()
        t = self.two(j, HERE, HERE) + self.r1[j, 0].astype(F32) + self.r2[j].astype(F32)
        if j == 0:
            self.fin[...] = t
        else:
            self.own[j, HERE, HERE] = t.astype(BF16)
            self.hop3(j).start()

    def total(self):
        t = self.fin[...]
        for j in ZS:
            self.hop3(j).wait_recv()
            t = t + self.r3[j - 1].astype(F32)
        return t.astype(BF16)

    def end(self):
        for j in range(4):
            for f in CORES:
                for s in CORES:
                    self.give(j, f, s).wait_send()
            self.hop1(j).wait_send()
            self.hop2(j).wait_send()
            if j:
                self.hop3(j).wait_send()


def scatter_steps(p, sets):
    def at(*does):
        return lambda: [over(p, sets, d) for d in does] and None

    begin = [at(*[lambda u, j=j: u.begin(j, u.load) for j in FAR]), at(*[lambda u, j=j: u.begin(j, u.give) for j in FAR])]
    steps = []
    for i in range(len(FAR) + 2):
        does = [(lambda u, j=FAR[i - back], w=w: getattr(u, w)(j)) for back, w in enumerate(("step1", "step2", "step3")) if 0 <= i - back < len(FAR)]
        steps += [at(d) for d in does]
    return begin, steps


def buffers(name):
    cut = cuts(name, 0)
    r, c = cut[0].size[0], sum(x.size[1] for x in cut)
    return [regs((*lead, r, c), t) for lead, t in zip(map(ints, ("4,2,2", "4,2,2", "4,2", "4", "3")), 5 * [BF16])] + [regs((r, c), F32)]


SWAPPED = dict(q=512, kv=HEAD, gu=FF)
KEPT = dict(q=[HEADS * HEAD], kv=[HEAD] * 2, gu=[FF] * 2)


class ScatterJob(Job):
    wait = ints("0,1")

    def __init__(self, grads):
        self.names = tuple(grads)
        n = count(self.names)
        self.ins = [(g.reshape(full_shape(k)), HBM) for k, g in grads.items()]
        self.outs, self.scratch = [], []
        for k in self.names:
            rows = ROWS[k] // 2
            self.outs += [(jax.ShapeDtypeStruct((rows, c), BF16), VMEM) for c in KEPT.get(k, [D])]
            self.scratch += buffers(k)
            if k in SWAPPED:
                self.scratch += [regs((2, ROWS[k], SWAPPED[k]), BF16)]
            if k == "d":
                self.scratch += [regs((2, 8, D), BF16)]
        self.scratch += [dma((n, Scatter.SENDS)), dma((n, Scatter.SENDS)), dma((n, Scatter.LOADS)), dma((n,)), dma((n,))]

    def split(self, refs):
        refs = list(refs)
        take = lambda n: [refs.pop(0) for _ in range(n)]
        full = dict(zip(self.names, take(len(self.names))))
        outs = {k: take(len(KEPT.get(k, [D]))) for k in self.names}
        bufs, swap = {}, {}
        for k in self.names:
            bufs[k] = take(6)
            if k in SWAPPED or k == "d":
                swap[k] = take(1)[0]
        return full, outs, bufs, swap, refs

    def prepare(self, p, refs):
        full, outs, bufs, swap, sems = self.split(refs)

        def make(n, name, i, c):
            cut, far = cuts(name, c)[i], cuts(name, 1 - c)[i]
            trim = lambda b, cut: b.at[..., : cut.size[0], pl.ds(*cut.span)]
            return Scatter(p, n, name, full[name], cut, far, [trim(b, cut) for b in bufs[name]], trim(bufs[name][1], far), sems[:3])

        sets = deal(p, self.names, make)
        (self.before, self.start), self.steps = scatter_steps(p, sets)
        self.end = lambda: self.keep(p, sets, outs, swap, sems[3:])

    def keep(self, p, sets, outs, swap, sem):
        units, low = sets
        swaps = {}
        for k in self.names:
            mine = [u for u in units if u.name == k]
            for u in mine:
                at = pl.ds(*u.cols)
                if k in SWAPPED:
                    swap[k][0, :, at] = u.total()
                else:
                    outs[k][0][:, at] = u.total()
            if k in SWAPPED:
                swaps[k] = send(swap[k].at[0], swap[k].at[1], sem, mine[0].n, p.partner)
                swaps[k].start()
        if "d" in swap:
            out, both, rows = outs["d"][0], swap["d"], D_CUT[0][1]
            n = low[0][0].n
            c = send(both.at[0], both.at[1], sem, n, p.partner)

            @pl.when(p.core == 0)
            def _():
                t = low[0][0].total()
                both[0] = t[rows - 8 :]
                c.start()
                out[...] = t[: out.shape[0]]
                c.wait_send()
                low[0][0].end()

            @pl.when(p.core == 1)
            def _():
                out[4:] = low[1][0].total()
                c.wait_recv()
                out[:4] = both[1, 4:]
                low[1][0].end()

        for k, c in swaps.items():
            c.wait()
            for core in CORES:

                @pl.when(p.core == core)
                def _():
                    rows = pl.ds(core * ROWS[k] // 2, ROWS[k] // 2)
                    for i in CORES:
                        part = swap[k][0 if i == core else 1, rows, :]
                        if k == "q":
                            outs[k][0][:, pl.ds(i * SWAPPED[k], SWAPPED[k])] = part
                        else:
                            outs[k][i][...] = part

        for u in units:
            u.end()

    def results(self, outs):
        outs = list(outs)
        return {k: [outs.pop(0) for _ in KEPT.get(k, [D])] for k in self.names}


def solution(mesh):
    cos, sin = rope_tables()

    def step(x, dy, *weights):
        blocks = prep(weights)
        of = lambda n, *names: {k: blocks[k][n] for k in names}
        ids = iter(range(1, 100))
        h, kept, w = x[0], [], [{}, {}]
        _, w[0] = call(nothing, 1, [], [], link=(GatherJob(of(0, "q", "kv")), next(ids)))
        for n in CORES:
            if n == 0:
                (q, k, v), more = qkv(h, w[n], cos, sin, (GatherJob(of(n, "o", "d")), next(ids)))
                w[n].update(more)
            else:
                q, k, v = qkv(h, w[n], cos, sin)
            (o, lse), more = attend(q, k, v, (GatherJob(of(n, "gu")), next(ids)))
            w[n].update(more)
            if n == 0:
                (mid, out), w[1] = after(o, h, w[n], (GatherJob(of(1, "q", "kv", "o", "d")), next(ids)))
            else:
                mid, out = after(o, h, w[n])
            kept.append((h, q, k, v, o, lse, mid))
            h = out
        by, grads, last = dy[0], [{}, {}], None
        for n in (1, 0):
            h, q, k, v, o, lse, mid = kept[n]
            if n == 1:
                bymid, byo, delta, ggu, gd, go = after_back(by, mid, o, w[n])
            else:
                (bymid, byo, delta, ggu, gd, go), more = after_back(by, mid, o, w[n], (ScatterJob(last), next(ids)))
                grads[1].update(more)
            big = dict(gu=ggu, d=gd) if n == 1 else dict(gu=ggu, d=gd, o=go)
            (dq, dk, dv), more = attend_back(q, k, v, byo, lse, delta, (ScatterJob(big), next(ids)))
            grads[n].update(more)
            by, gq, gkv = qkv_back(dq, dk, dv, h, bymid, w[n], cos, sin)
            last = dict(q=gq, kv=gkv, o=go) if n == 1 else dict(q=gq, kv=gkv)
        _, more = call(nothing, 1, [], [], link=(ScatterJob(last), next(ids)))
        grads[0].update(more)
        return (by[None], *(jnp.stack([g[k][i] for g in grads]) for k, i in (("q", 0), ("kv", 0), ("kv", 1), ("o", 0), ("gu", 0), ("gu", 1), ("d", 0))))

    states, cut = P(("rep", "dp"), None, None), P(None, "dp", None)
    return jax.shard_map(step, mesh=mesh, in_specs=(states, states) + (cut,) * 7, out_specs=(states,) + (P("rep", "dp", None),) * 7, check_vma=False)
```

```python
import collections

import jax
import jax.numpy as jnp
import numpy as np
from jax import lax
from jax.experimental import pallas as pl
from jax.experimental.pallas import tpu as pltpu
from jax.sharding import PartitionSpec as P


def ints(text):
    return tuple(map(int, text.split(",")))


D, HEADS, HEAD, FF, TOKENS, THETA = ints("640,8,128,3200,2048,10000")
FFS = tuple(map(ints, ("0,768", "768,768", "1536,768", "2304,896")))
BK = 512
SCALE, LOG2E, HIDDEN = HEAD**-0.5, 1.4426950408889634, -2e30
F32, BF16 = jnp.float32, jnp.bfloat16
CORES = HERE, THERE = (0, 1)
VMEM_MAX = 63 * 2**20


def dot(a, b, ca=1, cb=0):
    return lax.dot_general(a, b, (((ca,), (cb,)), ((), ())), preferred_element_type=F32)


def dot_t(a, b):
    return dot(a, b, 1, 1)


def rope_tables():
    half = HEAD // 2
    rate = np.float32(THETA) ** (-np.arange(half, dtype=np.float32) / np.float32(half))
    angle = (np.arange(TOKENS, dtype=np.float32)[:, None] * rate).astype(np.float64)
    cos, sin = np.cos(angle), np.sin(angle)
    return np.concatenate([cos, cos], 1).astype(np.float32), np.concatenate([-sin, sin], 1).astype(np.float32)


def norm(h):
    wide = h.astype(F32)
    scale = lax.rsqrt(jnp.mean(wide * wide, -1, keepdims=True) + 1e-6)
    return wide, scale, (wide * scale).astype(BF16)


def norm_back(wide, scale, by):
    return (scale * by - wide * (scale * scale * scale * jnp.mean(by * wide, -1, keepdims=True))).astype(BF16)


def turn(t, cos, sin):
    return t * cos + pltpu.roll(t, HEAD // 2, 1) * sin


def turn_back(t, cos, sin):
    return t * cos + pltpu.roll(t * sin, HEAD // 2, 1)


def whole(*shape):
    return pl.BlockSpec(shape, lambda *_: (0,) * len(shape), pipeline_mode=pl.Buffered(1))


def rows(t, n=D):
    return pl.BlockSpec((t, n), lambda i: (i, 0))


def heads(t, at=lambda i: i):
    return pl.BlockSpec((HEADS, t, HEAD), lambda i: (0, at(i), 0))


def stats(t, at=lambda i: i):
    return pl.BlockSpec((HEADS, t), lambda i: (0, at(i)))


def like(*shape, t=BF16):
    return jax.ShapeDtypeStruct(shape, t)


def nothing(*_):
    pass


def call(body, grid, ins, outs, scratch=(), link=(), stops=1, flops=0, exps=0):
    job = link[0] if link else ()
    xins, xouts, xscratch = (job.ins, job.outs, job.scratch) if link else ((), (), ())
    sizes = [len(ins), len(xins), len(outs), len(xouts), len(scratch), len(xscratch)]

    def kernel(*refs):
        groups = []
        for n in sizes:
            groups.append(refs[:n])
            refs = refs[n:]
        ours, more = [sum(groups[i::2], ()) for i in CORES]
        step = pl.program_id(0)
        if link:
            job.begin(step, more, grid, stops)
        body(step, job.stop if link else nothing, *ours)
        if link:
            job.finish()

    got = call_plain(kernel, grid, [*ins, *xins], [*outs, *xouts], [*scratch, *xscratch], link[1] if link else None, flops, exps)
    n = sizes[2]
    return (got[:n], job.results(got[n:])) if link else got


def call_plain(kernel, grid, ins, outs, scratch, cid=None, flops=0, exps=0):
    moved = sum(a.size * a.dtype.itemsize for a in (*[i[0] for i in ins], *[o[0] for o in outs]))
    params = {} if cid is None else dict(collective_id=cid, has_side_effects=True)
    return pl.pallas_call(
        kernel,
        grid=(grid,),
        in_specs=[i[1] for i in ins],
        out_specs=[o[1] for o in outs],
        out_shape=[o[0] for o in outs],
        scratch_shapes=scratch,
        compiler_params=pltpu.CompilerParams(dimension_semantics=("arbitrary",), vmem_limit_bytes=VMEM_MAX, **params),
        cost_estimate=pl.CostEstimate(flops=flops, transcendentals=exps, bytes_accessed=moved),
    )(*[i[0] for i in ins])


def qkv_rows(h, wq_ref, wkv_ref, cos, sin, q_ref, k_ref, v_ref):
    _, _, a = norm(h)
    q = dot(a, wq_ref[...]).astype(BF16).astype(F32)
    for n in range(HEADS):
        q_ref[n] = turn(q[:, n * HEAD : (n + 1) * HEAD], cos, sin).astype(BF16)
    k_ref[...] = turn(dot(a, wkv_ref[HERE]).astype(BF16).astype(F32), cos, sin).astype(BF16)
    v_ref[...] = dot(a, wkv_ref[THERE]).astype(BF16)


def joined(o_ref):
    return jnp.concatenate([o_ref[n] for n in range(HEADS)], axis=1)


def weights_of(w):
    return [(w["o"], whole(HEADS * HEAD, D)), (w["gu"], whole(2, D, FF)), (w["d"], whole(FF, D))]


def middle(o, h, wo_ref):
    return h + dot(o, wo_ref[...]).astype(BF16)


def hidden_rows(mid, wgu_ref, p_ref):
    _, _, b = norm(mid)
    for at, n in FFS:
        part = pl.ds(at, n)
        gate, up = (dot(b, wgu_ref[i, :, part]) for i in CORES)
        p_ref[:, part] = (gate * jax.nn.sigmoid(gate) * up).astype(BF16)


def after_back(by, mid, o, w, link=(), fresh=False, t=256):
    grid = TOKENS // t
    pieces, most = FF // D, D

    def body(step, stop, by_ref, mid_ref, o_ref, wo_ref, wgu_ref, wd_ref, bymid_ref, byo_ref, delta_ref, gu_hbm, d_hbm, o_hbm,
             acc_gu, acc_d, acc_o, st_gu, st_d, st_o, sem_gu, sem_d, sem_o):
        first, last = step == 0, step == grid - 1
        by = by_ref[...]
        o = joined(o_ref)
        wide, scale, b = norm(middle(o, mid_ref[...], wo_ref) if fresh else mid_ref[...])
        bt, byt = b.T, by.T

        def add(ref, v):
            ref[...] = jnp.where(first, 0.0, ref[...]) + v

        def leaving(i):
            at = pl.ds(i * most, most)
            return [pltpu.make_async_copy(st_gu.at[i % 2], gu_hbm.at[:, :, at], sem_gu.at[i % 2]),
                    pltpu.make_async_copy(st_d.at[i % 2], d_hbm.at[at, :], sem_d.at[i % 2])]

        def ahead(at, n):
            part = pl.ds(at, n)
            return [dot(b, wgu_ref[i, :, part]) for i in CORES] + [dot_t(by, wd_ref[part, :])]

        byb = 0.0
        coming = ahead(*FFS[0])
        for k, (at, n) in enumerate(FFS):
            gate, up, byp = coming
            if k + 1 < len(FFS):
                coming = ahead(*FFS[k + 1])
            part = pl.ds(at, n)
            byp = byp.astype(BF16).astype(F32)
            s = jax.nn.sigmoid(gate)
            silu = gate * s
            bys = (byp * up * (s + silu * (1.0 - s))).astype(BF16), (byp * silu).astype(BF16)
            add(acc_d.at[:, part], dot(byt, (silu * up).astype(BF16)))
            for i in CORES:
                add(acc_gu.at[i, :, part], dot(bt, bys[i]))
                byb += dot_t(bys[i], wgu_ref[i, :, part])

        bymid = by + norm_back(wide, scale, byb.astype(BF16).astype(F32))
        bymid_ref[...] = bymid
        byo = dot_t(bymid, wo_ref[...]).astype(BF16)
        add(acc_o, dot(o.T, bymid))
        for n in range(HEADS):
            one = slice(n * HEAD, (n + 1) * HEAD)
            byo_ref[n] = byo[:, one]
            delta_ref[n : n + 1, :] = (byo[:, one].astype(F32) * o[:, one].astype(F32)).T.sum(0, keepdims=True)

        @pl.when(last)
        def _():
            st_o[...] = acc_o[...].astype(BF16)
            c = pltpu.make_async_copy(st_o, o_hbm, sem_o)
            c.start()
            for i in range(pieces):
                piece = pl.ds(i * most, most)
                if i > 1:
                    for x in leaving(i - 2):
                        x.wait()
                st_gu[i % 2] = acc_gu[:, :, piece].astype(BF16)
                st_d[i % 2] = acc_d[:, piece].T.astype(BF16)
                for x in leaving(i):
                    x.start()
            for x in (*leaving(pieces - 2), *leaving(pieces - 1), c):
                x.wait()

    ins = [(by, rows(t)), (mid, rows(t)), (o, heads(t)), *weights_of(w)]
    outs = [(like(TOKENS, D), rows(t)), (like(HEADS, TOKENS, HEAD), heads(t)), (like(HEADS, TOKENS, t=F32), stats(t)),
            (like(2, D, FF), HBM), (like(FF, D), HBM), (like(HEADS * HEAD, D), HBM)]
    scratch = [regs((2, D, FF), F32), regs((D, FF), F32), regs((HEADS * HEAD, D), F32), regs((2, 2, D, most), BF16), regs((2, most, D), BF16),
               regs((HEADS * HEAD, D), BF16), dma((2,)), dma((2,)), dma]
    return call(body, grid, ins, outs, scratch, link, flops=2 * TOKENS * D * (2 * HEADS * HEAD + 8 * FF))


def qkv_back(dq, dk, dv, h, bymid, w, cos, sin, link=(), t=1024):
    grid = TOKENS // t

    def body(step, stop, dq_ref, dk_ref, dv_ref, h_ref, bymid_ref, wq_ref, wkv_ref, cos_ref, sin_ref, byh_ref, gq_ref, gkv_ref, acc_q, acc_kv):
        first, last = step == 0, step == grid - 1
        cos, sin = cos_ref[...], sin_ref[...]
        wide, scale, a = norm(h_ref[...])
        at = a.T
        dq = jnp.concatenate([turn_back(dq_ref[n].astype(F32), cos, sin).astype(BF16) for n in range(HEADS)], axis=1)
        dkv = turn_back(dk_ref[...].astype(F32), cos, sin).astype(BF16), dv_ref[...]
        acc_q[...] = jnp.where(first, 0.0, acc_q[...]) + dot(at, dq)
        bya = dot_t(dq, wq_ref[...])
        for i in CORES:
            acc_kv[i] = jnp.where(first, 0.0, acc_kv[i]) + dot(at, dkv[i])
            bya += dot_t(dkv[i], wkv_ref[i])
        byh_ref[...] = bymid_ref[...] + norm_back(wide, scale, bya.astype(BF16).astype(F32))

        @pl.when(last)
        def _():
            gq_ref[...] = acc_q[...].astype(BF16)
            gkv_ref[...] = acc_kv[...].astype(BF16)

    wq, wkv = whole(D, HEADS * HEAD), whole(2, D, HEAD)
    ins = [(dq, heads(t)), (dk, rows(t, HEAD)), (dv, rows(t, HEAD)), (h, rows(t)), (bymid, rows(t)), (w["q"], wq), (w["kv"], wkv), (cos, rows(t, HEAD)), (sin, rows(t, HEAD))]
    outs = [(like(TOKENS, D), rows(t)), (like(D, HEADS * HEAD), wq), (like(2, D, HEAD), wkv)]
    scratch = [regs((D, HEADS * HEAD), F32), regs((2, D, HEAD), F32)]
    return call(body, grid, ins, outs, scratch, link, flops=4 * TOKENS * D * (HEADS + 2) * HEAD)


def fwd_place(s):
    iq = sum(jnp.minimum(s // n, 1) for n in ints("1,3,6"))
    return iq, s - iq * (iq + 1) // 2


def attend_block(iq, jk, q_ref, k_ref, v_ref, o_ref, lse_ref, top_s, mix_s):
    e = SCALE * LOG2E

    @pl.when(jk == 0)
    def _():
        top_s[...] = jnp.full(top_s.shape, HIDDEN / 2, F32)
        mix_s[...] = jnp.zeros(mix_s.shape, F32)

    def block(masked):
        k = k_ref[...]
        values = jnp.concatenate([v_ref[...].T, jnp.ones((8, BK), BF16)], axis=0)
        scores = [dot_t(k, q_ref[n]) for n in range(HEADS)]
        weights, keeps = [], []
        for n, x in enumerate(scores):
            if masked:
                x = jnp.where(lax.broadcasted_iota(jnp.int32, x.shape, 1) >= lax.broadcasted_iota(jnp.int32, x.shape, 0), x, HIDDEN)
            one = slice(n, n + 1)
            old = top_s[one, :]
            top = jnp.maximum(old, x.max(axis=0, keepdims=True))
            top_s[one, :] = top
            weights.append(jnp.exp2((x - top) * e).astype(BF16))
            keeps.append(jnp.exp2((old - top) * e))
        for n, (p, keep) in enumerate(zip(weights, keeps)):
            mix_s[n] = mix_s[n] * keep + dot(values, p)

    pl.when(jk < iq)(lambda: block(False))

    @pl.when(jk == iq)
    def _():
        block(True)
        for n in range(HEADS):
            total = mix_s[n, HEAD : HEAD + 1, :]
            o_ref[n] = (mix_s[n, :HEAD, :] * (1.0 / total)).T.astype(BF16)
            lse_ref[n : n + 1, :] = top_s[n : n + 1, :] * SCALE + jnp.log(total)


QKVS, PAIRS, HIDDENS, DOWNS = ints("4,10,8,4")
MLP = QKVS + PAIRS
DOWN = MLP + HIDDENS
LAYER = DOWN + DOWNS
FORWARD = LAYER + QKVS + PAIRS


def forward(x, blocks, cos, sin, cid):
    names = list(ROWS)
    saved = dict(q=(HEADS, TOKENS, HEAD), k=(TOKENS, HEAD), v=(TOKENS, HEAD), o=(HEADS, TOKENS, HEAD), lse=(HEADS, TOKENS))
    kinds = {k: F32 if k == "lse" else BF16 for k in saved}
    sizes = [len(ROWS) * 2, 3, len(ROWS) * 2, 2, 2 * len(saved), 3, len(saved), len(ROWS), 3, 3]

    def body(*refs):
        refs = list(refs)
        bs, (x_hbm, cos_ref, sin_ref), fulls, (mid_hbm, h_hbm), kept, (h_s, p_s, top_s), temps, ws, gsems, (mix_s, wsem, ksem) = (
            [refs.pop(0) for _ in range(n)] for n in sizes)
        step = pl.program_id(0)
        p = Place()
        of = lambda refs, layer: {n: refs[2 * i + layer] for i, n in enumerate(names)}
        w, kept, temp = dict(zip(names, ws)), [dict(zip(saved, kept[i::2])) for i in CORES], dict(zip(saved, temps))
        sets, first = [], 0
        for layer in CORES:
            for group in (("q", "kv"), ("gu", "o"), ("d",)) if layer == HERE else (("q", "kv"), ("gu", "o", "d")):
                sets.append(gather_steps(p, gather_sets(p, group, of(fulls, layer), of(bs, layer), gsems, first)))
                first += count(group)

        def loads(layer, some):
            return [pltpu.make_async_copy(of(fulls, layer)[n], w[n].at[layer] if n in ("q", "kv") else w[n], wsem.at[names.index(n), layer]) for n in some]

        def keeps(layer, some):
            return [pltpu.make_async_copy(temp[n], kept[layer][n], ksem.at[list(saved).index(n), layer]) for n in some]

        states = [pltpu.make_async_copy(x_hbm, h_s, ksem.at[len(saved), HERE]), pltpu.make_async_copy(h_s, mid_hbm, ksem.at[len(saved), THERE]),
                  pltpu.make_async_copy(h_s, h_hbm, ksem.at[len(saved) + 1, HERE])]
        start = lambda copies: [c.start() for c in copies]
        wait = lambda copies: [c.wait() for c in copies]
        early, late = ("q", "kv"), ("o", "gu")
        qkv_of, o_of = ("q", "k", "v"), ("o", "lse")
        s1, s2, s2d, s3, s4 = sets
        plan = collections.defaultdict(list)
        at = lambda place, *does: plan[place].extend(does)

        def lay(places, steps):
            for place, x in zip(ints(places), steps):
                at(place, x)

        at(HERE, lambda: greet(everyone(p)), lambda: start(states[:1]))
        lay("0,0,0,0,0,0", (s1.start_z, s1.start_xy, s2.start_z, s2.start_xy, s2d.start_z, s2d.start_xy))
        at(HERE, *s1.steps, s1.finish, lambda: start(loads(HERE, early)), *s2.steps[:2], lambda: wait(loads(HERE, early) + states[:1]))
        lay("3,4,7,9,10,11,13,14", (*s2.steps[2:], s2.finish))
        lay("8,8,10,10,12,13,14,16,18,21", (*s2d.steps, s2d.finish))
        at(QKVS, lambda: start(keeps(HERE, qkv_of)))
        lay("10,10,14,14", (s3.start_z, s4.start_z, s3.start_xy, s4.start_xy))
        lay("14,15,16,17,18,19,20,21,22,23,24", (*s3.steps, s3.finish, lambda: start(loads(THERE, early))))
        lay("18,18,21,22,26,27,29,34,37", s4.steps)
        at(MLP, lambda: start(loads(HERE, late)), lambda: start(keeps(HERE, o_of)), lambda: wait(loads(HERE, late)))
        at(DOWN - 1, lambda: start(loads(HERE, ("d",))))
        at(DOWN, lambda: start(states[1:2]), lambda: wait(loads(HERE, ("d",)) + states[1:2]))
        at(LAYER, lambda: start(states[2:]), lambda: wait(loads(THERE, early) + keeps(HERE, qkv_of + o_of)))
        at(LAYER + QKVS, lambda: start(keeps(THERE, qkv_of)))
        for place, does in sorted(plan.items()):

            @pl.when(step == place)
            def _():
                for do in does:
                    do()

        layer = jnp.minimum(step // LAYER, 1)
        t = step - layer * LAYER

        @pl.when(t < QKVS)
        def _():
            n = TOKENS // QKVS
            rows = pl.ds(pl.multiple_of(t * n, n), n)
            qkv_rows(h_s[rows, :], w["q"].at[layer], w["kv"].at[layer], cos_ref[rows, :], sin_ref[rows, :], temp["q"].at[:, rows, :], temp["k"].at[rows, :],
                     temp["v"].at[rows, :])

        @pl.when((t >= QKVS) & (t < MLP))
        def _():
            iq, jk = fwd_place(t - QKVS)
            rows, keys = (pl.ds(pl.multiple_of(i * BK, BK), BK) for i in (iq, jk))
            attend_block(iq, jk, temp["q"].at[:, rows, :], temp["k"].at[keys, :], temp["v"].at[keys, :], temp["o"].at[:, rows, :], temp["lse"].at[:, rows],
                         top_s, mix_s)

        def rows_of(first, many):
            n = TOKENS // many
            return pl.ds(pl.multiple_of((t - first) * n, n), n)

        @pl.when((t >= MLP) & (t < DOWN))
        def _():
            rows = rows_of(MLP, HIDDENS)
            o = jnp.concatenate([temp["o"][i, rows, :] for i in range(HEADS)], axis=1)
            mid = middle(o, h_s[rows, :], w["o"])
            h_s[rows, :] = mid
            hidden_rows(mid, w["gu"], p_s.at[rows, :])

        @pl.when(t >= DOWN)
        def _():
            rows = rows_of(DOWN, DOWNS)
            h_s[rows, :] += dot(p_s[rows, :], w["d"][...]).astype(BF16)

        @pl.when(step == FORWARD - 1)
        def _():
            start(keeps(THERE, o_of))
            s4.finish()
            wait(keeps(THERE, qkv_of + o_of) + states[2:])

    ins = [(b, VMEM) for n in names for b in blocks[n]] + [(x, HBM), (cos, whole(TOKENS, HEAD)), (sin, whole(TOKENS, HEAD))]
    outs = [(like(*LEAD[n], CHIPS * ROWS[n], COLS[n]), HBM) for n in names for _ in CORES] + [(like(TOKENS, D), HBM)] * 2
    outs += [(like(*s, t=kinds[k]), HBM) for k, s in saved.items() for _ in CORES]
    units = 2 * count(names)
    weights = [regs((*([2] if n in ("q", "kv") else []), *LEAD[n], CHIPS * ROWS[n], COLS[n]), BF16) for n in names]
    scratch = [regs((TOKENS, D), BF16), regs((TOKENS, FF), BF16), regs((HEADS, BK), F32), *[regs(s, kinds[k]) for k, s in saved.items()], *weights,
               dma((units, Gather.SENDS)), dma((units, Gather.SENDS)), dma((units,)), regs((HEADS, HEAD + 8, BK), F32), dma((len(names), 2)),
               dma((len(saved) + 2, 2))]
    got = list(call_plain(body, FORWARD, ins, outs, scratch, cid, flops=2 * TOKENS * D * (3 * FF + HEADS * HEAD * 6)))
    take = lambda n: [got.pop(0) for _ in range(n)]
    full = take(2 * len(names))
    w = [{n: full[2 * i + layer] for i, n in enumerate(names)} for layer in CORES]
    mid, h = take(2)
    return w, mid, h, [got[i::2] for i in CORES]


def back_place(s):
    g = sum(jnp.minimum(s // n, 1) for n in ints("2,6,12"))
    r = s - g * (g + 1)
    second = jnp.minimum(r // (g + 1), 1)
    return g, 2 * g + second, r - second * (g + 1)


def attend_back(q, k, v, byo, lse, delta, link=()):
    blocks, e, bq = 20, SCALE * LOG2E, BK // 2
    at = lambda s: back_place(s)[1]
    pairs = range(0, HEADS, 2)

    def body(s, stop, q_ref, k_ref, v_ref, do_ref, lse_ref, delta_ref, dq_ref, dk_ref, dv_ref, dq_s, dk_s, dv_s):
        g, iq, jk = back_place(s)
        keys = pl.ds(pl.multiple_of(jk * BK, BK), BK)
        row = lambda ref, n: jnp.concatenate([ref[n : n + 1, :], ref[n + 1 : n + 2, :]], axis=1)

        @pl.when(s == 0)
        def _():
            dk_s[...] = jnp.zeros(dk_s.shape, F32)
            dv_s[...] = jnp.zeros(dv_s.shape, F32)

        @pl.when(jk == 0)
        def _():
            dq_s[...] = jnp.zeros(dq_s.shape, F32)

        def block(masked):
            k, v = k_ref[keys, :], v_ref[keys, :]
            kt = k.T
            qs = [q_ref[n : n + 2].reshape(2 * bq, HEAD) for n in pairs]
            dos = [do_ref[n : n + 2].reshape(2 * bq, HEAD) for n in pairs]
            scores = [dot_t(k, x) for x in qs]
            dps = [dot_t(v, x) for x in dos]
            for i, n in enumerate(pairs):
                p = jnp.exp2(scores[i] * e - row(lse_ref, n) * LOG2E)
                if masked:
                    ahead = lax.rem(lax.broadcasted_iota(jnp.int32, p.shape, 1), bq) - lax.broadcasted_iota(jnp.int32, p.shape, 0)
                    p = jnp.where(ahead >= jk * BK - iq * bq, p, 0.0)
                ds = (p * (dps[i] - row(delta_ref, n))).astype(BF16)
                dv_s[keys, :] += dot(p.astype(BF16), dos[i])
                dk_s[keys, :] += dot(ds, qs[i])
                dq_s[n // 2] += dot(kt, ds)

        def last():
            block(True)
            for n in pairs:
                dq_ref[n : n + 2] = (dq_s[n // 2] * SCALE).T.reshape(2, bq, HEAD).astype(BF16)

        pl.when(jk < g)(lambda: block(False))
        pl.when(jk == g)(last)

        @pl.when(s == blocks - 1)
        def _():
            dk_ref[...] = (dk_s[...] * SCALE).astype(BF16)
            dv_ref[...] = dv_s[...].astype(BF16)

    kv = whole(TOKENS, HEAD)
    return call(body, blocks, [(q, heads(bq, at)), (k, kv), (v, kv), (byo, heads(bq, at)), (lse, stats(bq, at)), (delta, stats(bq, at))],
                [(like(HEADS, TOKENS, HEAD), heads(bq, at)), *[(like(TOKENS, HEAD), kv)] * 2],
                [regs((HEADS // 2, HEAD, BK), F32), regs((TOKENS, HEAD), F32), regs((TOKENS, HEAD), F32)], link,
                flops=blocks * 5 * BK * BK * HEADS * HEAD, exps=blocks * BK * bq * HEADS)


def prep(wq, wk, wv, wo, wg, wu, wd):
    names = list(ROWS)
    arrays = [jnp.concatenate([wq, wk, wv, wg, wu], axis=2), wo, wd]
    parts, at = [], 0
    for name in ("q", "kv", "gu"):
        for lead in [(c,) for c in CORES] if LEAD[name] else [()]:
            parts.append((0, name, lead, at))
            at += COLS[name]
    parts += [(1, "o", (), 0), (2, "d", (), 0)]

    def kernel(*refs):
        refs = list(refs)
        own, blocks, here, there, sem = ([refs.pop(0) for _ in range(n)] for n in (len(arrays), 2 * len(names), len(arrays), len(arrays), len(ZS)))
        p = Place()
        local = [pltpu.make_async_copy(a, b, sem[2].at[i]) for i, (a, b) in enumerate(zip(own, here))]
        for c in local:
            c.start()
        greet([p.partner])
        far = [send(a, b, sem, i, p.partner) for i, (a, b) in enumerate(zip(own, there))]
        for c in far:
            c.start()
        for c in (*local, *far):
            c.wait()
        for core in CORES:

            @pl.when(p.core == core)
            def _():
                for i, name, lead, first in parts:
                    n, cols = ROWS[name] // 2, pl.ds(first, COLS[name])
                    for layer in CORES:
                        out = blocks[2 * names.index(name) + layer]
                        for to, src in ((core, here[i]), (1 - core, there[i])):
                            out[(*lead, pl.ds(to * n, n), ALL)] = src[layer, :, cols]

    got = pl.pallas_call(
        kernel,
        in_specs=[HBM] * len(arrays),
        out_specs=[VMEM] * 2 * len(names),
        out_shape=[like(*LEAD[n], ROWS[n], COLS[n]) for n in names for _ in CORES],
        scratch_shapes=[regs(w.shape, BF16) for w in arrays] * 2 + [dma((len(arrays),))] * len(ZS),
        compiler_params=pltpu.CompilerParams(collective_id=0, has_side_effects=True, vmem_limit_bytes=VMEM_MAX),
        name="prep",
    )(*arrays)
    return {n: got[2 * i : 2 * i + 2] for i, n in enumerate(names)}


MESH = pl.DeviceIdType.MESH
ZS = ints("1,2,3")
NEAR = ints("1,3,2")
FAR = ints("2,1,3,0")
BLOCKS = ints("2,2,4")
ALL = slice(None)
HBM, VMEM = pl.BlockSpec(memory_space=pltpu.HBM), pl.BlockSpec(memory_space=pltpu.VMEM)
dma, regs = pltpu.SemaphoreType.DMA, pltpu.VMEM


class Place:
    def __init__(self):
        me = self.me = lax.axis_index("dp")
        chip = me // 2
        self.core, self.z, self.y, self.x = me % 2, chip % 4, chip // 4 % 2, chip // 8
        self.partner = me + 1 - 2 * self.core
        self.side = {"x": me + 16 * (1 - 2 * self.x), "y": me + 8 * (1 - 2 * self.y)}

    def zat(self, j):
        return (self.z + j + 4) % 4

    def zn(self, j):
        return self.me + 2 * (self.zat(j) - self.z)

    def at(self, order, f, s, j):
        own = dict(x=self.x, y=self.y)
        for a, other in zip(order, (f, s)):
            own[a] = 1 - own[a] if other else own[a]
        return own["x"], own["y"], self.zat(j)


def greet(peers):
    barrier = pltpu.get_barrier_semaphore()
    for p in peers:
        pl.semaphore_signal(barrier, inc=1, device_id=(0, p), device_id_type=MESH)
    pl.semaphore_wait(barrier, len(peers))


def everyone(p):
    return [p.partner, *p.side.values()] + [p.zn(j) for j in ZS]


def send(src, dst, sem, i, to):
    return pltpu.make_async_remote_copy(src_ref=src, dst_ref=dst, send_sem=sem[0].at[i], recv_sem=sem[1].at[i], device_id=(0, to), device_id_type=MESH)


CHIPS = 16
ROWS = {k: n // CHIPS for k, n in dict(q=D, kv=D, o=HEADS * HEAD, gu=D, d=FF).items()}
COLS = dict(q=HEADS * HEAD, kv=HEAD, gu=FF, o=D, d=D)
LEAD = dict(q=(), kv=(2,), gu=(2,), o=(), d=())
ORDERS = ("yx", "xy")
GU_CUT = ints("0,1536"), ints("1536,1664")
LOW_CUT = ints("0,384"), ints("384,256")
Cut = collections.namedtuple("Cut", "lead,cols,order,span")


def cuts(name, core):
    if name == "q":
        half = COLS[name] // 2
        return [Cut((), pl.ds(pl.multiple_of(core * half, half), half), ORDERS[THERE], (0, half))]
    if name == "kv":
        return [Cut((core,), ALL, ORDERS[HERE], (0, HEAD))]
    if name == "gu":
        return [Cut((core,), pl.ds(*c), o, c) for c, o in zip(GU_CUT, ORDERS)]
    return [Cut((), pl.ds(*LOW_CUT[core]), ORDERS[core], (0, LOW_CUT[core][1]))]


def deal(p, names, make):
    units, low, n = [], ([], []), 0
    for name in names:
        if name in ("o", "d"):
            for c in CORES:
                low[c].append(make(n, name, 0, c))
            n += 1
        else:
            for i in range(len(cuts(name, 0))):
                units.append(make(n, name, i, p.core))
                n += 1
    return units, low


def count(names):
    return sum(len(cuts(name, 0)) for name in names)


def over(p, sets, step):
    units, low = sets
    for u in units:
        step(u)
    for c in CORES:
        if low[c]:

            @pl.when(p.core == c)
            def _():
                for u in low[c]:
                    step(u)


class Gather:
    FIRST, SECOND, PARTNER, SENDS = ints("3,7,15,19")

    def __init__(self, p, n, name, full, block, cut, far, sems):
        self.p, self.order, self.sem, self.lsem = p, cut.order, [s.at[n] for s in sems[:2]], sems[2].at[n]
        rows = ROWS[name]

        def part(cut, first, many):
            return full.at[(*cut.lead, pl.ds(pl.multiple_of(first * rows, 8), many * rows), cut.cols)]

        def line(cut, f, s):
            x, y, _ = p.at(cut.order, f, s, 0)
            return (x * 2 + y) * 4

        self.at = lambda f, s, j: part(cut, line(cut, f, s) + p.zat(-j), 1)
        self.group = lambda f, s: part(cut, line(cut, f, s), 4)
        self.theirs = lambda f, s: part(far, line(far, f, s), 4)
        self.block = block.at[(*cut.lead, ALL, cut.cols)]

    def src(self, f, j):
        return self.at(f, HERE, j) if f or j else self.block

    def to_z(self, j):
        return send(self.block, self.at(HERE, HERE, HERE), self.sem, j - 1, self.p.zn(j))

    def to_first(self, j):
        return send(self.src(HERE, j), self.at(HERE, HERE, j), self.sem, self.FIRST + j, self.p.side[self.order[0]])

    def to_second(self, f, j):
        return send(self.src(f, j), self.at(f, HERE, j), self.sem, self.SECOND + 4 * f + j, self.p.side[self.order[1]])

    def to_partner(self, f, s):
        return send(self.group(f, s), self.group(f, s), self.sem, self.PARTNER + 2 * f + s, self.p.partner)

    def local(self):
        return pltpu.make_async_copy(self.block, self.at(HERE, HERE, HERE), self.lsem)

    def got(self, i, ref):
        send(ref, ref, self.sem, i, self.p.partner).wait_recv()

    def start_z(self, j):
        self.to_z(j).start()

    def start_xy(self):
        self.to_first(HERE).start()
        self.to_second(HERE, HERE).start()
        self.local().start()

    def from_z(self, j):
        self.got(j - 1, self.at(HERE, HERE, j))
        self.to_first(j).start()
        self.to_second(HERE, j).start()
        if j == NEAR[-1]:
            self.local().wait()
            self.to_partner(HERE, HERE).start()

    def from_first(self, j):
        self.got(self.FIRST + j, self.at(THERE, HERE, j))
        self.to_second(THERE, j).start()
        if j == NEAR[-1]:
            self.to_partner(THERE, HERE).start()

    def from_second(self, f):
        for j in range(4):
            self.got(self.SECOND + 4 * f + j, self.at(f, THERE, j))
        self.to_partner(f, THERE).start()

    def finish(self):
        for f in CORES:
            for s in CORES:
                self.got(self.PARTNER + 2 * f + s, self.theirs(f, s))
        for j in ZS:
            self.to_z(j).wait_send()
        for j in range(4):
            self.to_first(j).wait_send()
            for f in CORES:
                self.to_second(f, j).wait_send()
        for f in CORES:
            for s in CORES:
                self.to_partner(f, s).wait_send()


Steps = collections.namedtuple("Steps", "start_z,start_xy,steps,finish")


def gather_steps(p, sets):
    text = "z1,f0,z3,f1,z2,f3,f2,s0,s1"
    kinds = dict(z="from_z", f="from_first", s="from_second")
    do = lambda name, *args: lambda: over(p, sets, lambda u: getattr(u, name)(*args))
    begin = [do("start_z", j) for j in NEAR]
    return Steps(lambda: [b() for b in begin], do("start_xy"), [do(kinds[o[0]], *map(int, o[1:])) for o in text.split(",")], do("finish"))


def gather_sets(p, names, full, block, sems, first):
    return deal(p, names, lambda n, name, i, c: Gather(p, first + n, name, full[name], block[name], cuts(name, c)[i], cuts(name, 1 - c)[i], sems))


class Job:
    def begin(self, step, refs, grid, stops):
        self.step, self.grid, self.stops, self.at = step, grid, stops, 0
        p = self.p = Place()
        self.prepare(p, refs)

        @pl.when(step == 0)
        def _():
            self.before()
            greet(everyone(p))
            self.start()

        self.stop()

    def stop(self):
        places = self.grid * self.stops
        first = places * self.wait[0] // self.wait[1]
        for place in range(self.at, places, self.stops):
            mine = [x for i, x in enumerate(self.steps) if first + i * (places - first) // len(self.steps) == place]
            if mine:

                @pl.when(self.step == place // self.stops)
                def _():
                    for x in mine:
                        x()

        self.at += 1

    def finish(self):
        pl.when(self.step == self.grid - 1)(self.end)

    def before(self):
        pass


class Scatter:
    FIRST, SECOND, Z, SENDS = ints("4,8,12,15")

    def __init__(self, p, n, name, full, cut, far, bufs, far_part, sems):
        self.p, self.name, self.span, self.n = p, name, cut.span, n
        self.order, far_order = cut.order[::-1], far.order[::-1]
        self.sem, self.lsem = [s.at[n] for s in sems[:2]], sems[2].at[n]

        def line(cut, order, f, s):
            x, y, _ = p.at(order, f, s, 0)
            return full.at[(*cut.lead, pl.ds((x * 2 + y) * 4, 4), ALL, cut.cols)]

        self.own, self.part, self.r1, self.r2, self.r3, self.fin = bufs
        self.load = lambda f, s: pltpu.make_async_copy(line(cut, self.order, f, s), self.own.at[f, s], self.lsem.at[2 * f + s])
        self.give = lambda f, s: send(line(far, far_order, f, s), far_part.at[f, s], self.sem, 2 * f + s, p.partner)

    def hop1(self, j):
        return send(self.own.at[THERE, :, self.p.zat(j)], self.r1.at[j], self.sem, self.FIRST + j, self.p.side[self.order[0]])

    def hop2(self, j):
        return send(self.own.at[HERE, THERE, self.p.zat(j)], self.r2.at[j], self.sem, self.SECOND + j, self.p.side[self.order[1]])

    def hop3(self, j):
        return send(self.own.at[HERE, HERE, self.p.zat(j)], self.r3.at[j - 1], self.sem, self.Z + j - 1, self.p.zn(j))

    def two(self, j, f, s):
        if j == FAR[0]:
            self.load(f, s).wait()
            here = self.part.at[f, s]
            send(here, here, self.sem, 2 * f + s, self.p.partner).wait_recv()
        z = self.p.zat(j)
        return self.own[f, s, z].astype(F32) + self.part[f, s, z].astype(F32)

    def step1(self, j):
        for s in CORES:
            self.own[THERE, s, self.p.zat(j)] = self.two(j, THERE, s).astype(BF16)
        self.hop1(j).start()

    def step2(self, j):
        self.hop1(j).wait_recv()
        self.own[HERE, THERE, self.p.zat(j)] = (self.two(j, HERE, THERE) + self.r1[j, THERE].astype(F32)).astype(BF16)
        self.hop2(j).start()

    def step3(self, j):
        self.hop2(j).wait_recv()
        t = self.two(j, HERE, HERE) + self.r1[j, HERE].astype(F32) + self.r2[j].astype(F32)
        if j == HERE:
            self.fin[...] = t
        else:
            self.own[HERE, HERE, self.p.zat(j)] = t.astype(BF16)
            self.hop3(j).start()

    def total(self):
        t = self.fin[...]
        for j in ZS:
            self.hop3(j).wait_recv()
            t = t + self.r3[j - 1].astype(F32)
        return t.astype(BF16)

    def end(self):
        for f in CORES:
            for s in CORES:
                self.give(f, s).wait_send()
        for j in range(4):
            self.hop1(j).wait_send()
            self.hop2(j).wait_send()
        for j in ZS:
            self.hop3(j).wait_send()


def scatter_steps(p, sets):
    does = [lambda what=what: [over(p, sets, lambda u: getattr(u, what)(f, s).start()) for f in CORES[::-1] for s in CORES[::-1]] for what in ("load", "give")]
    steps = []
    for i in range(len(FAR) + 2):
        for back, w in enumerate(("step1", "step2", "step3")):
            if 0 <= i - back < len(FAR):
                steps.append(lambda j=FAR[i - back], w=w: over(p, sets, lambda u: getattr(u, w)(j)))
    return does, steps


WIDTH = dict(q=COLS["q"] // 2, kv=HEAD, gu=FF, o=LOW_CUT[0][1], d=LOW_CUT[0][1])
KEPT = dict(kv=[HEAD] * 2, gu=[FF] * 2)


def buffers(name):
    r, c = ROWS[name], WIDTH[name]
    shapes = [(*ints(lead), r, c) for lead in ("2,2,4", "2,2,4", "4,2", "4", "3")]
    return [regs(s, BF16) for s in shapes] + [regs((r, c), F32), regs((2, r, c), BF16)]


class ScatterJob(Job):
    wait = ints("0,1")

    def __init__(self, grads):
        self.names = tuple(grads)
        n = count(self.names)
        self.ins = [(g.reshape(*LEAD[k], CHIPS, ROWS[k], COLS[k]), HBM) for k, g in grads.items()]
        self.outs = [(jax.ShapeDtypeStruct((ROWS[k] // 2, c), BF16), VMEM) for k in self.names for c in KEPT.get(k, [COLS[k]])]
        self.scratch = sum(map(buffers, self.names), []) + [dma((n, Scatter.SENDS)), dma((n, Scatter.SENDS)), dma((n, 4)), dma((n,)), dma((n,))]

    def prepare(self, p, refs):
        refs = list(refs)
        take = lambda n: [refs.pop(0) for _ in range(n)]
        full = dict(zip(self.names, take(len(self.names))))
        outs = {k: take(len(KEPT.get(k, [D]))) for k in self.names}
        bufs = {k: take(len(buffers(k))) for k in self.names}

        def make(n, name, i, c):
            cut, far = cuts(name, c)[i], cuts(name, 1 - c)[i]
            trim = lambda b, cut: b.at[..., pl.ds(*cut.span)]
            return Scatter(p, n, name, full[name], cut, far, [trim(b, cut) for b in bufs[name][:-1]], trim(bufs[name][1], far), refs[:3])

        sets = deal(p, self.names, make)
        (self.before, self.start), self.steps = scatter_steps(p, sets)
        self.end = lambda: self.keep(p, sets, outs, {k: b[-1] for k, b in bufs.items()}, refs[3:])

    def keep(self, p, sets, outs, swap, sem):
        units, low = sets
        firsts = {}
        for u in (*units, *low[0]):
            firsts.setdefault(u.name, u)

        def change(k, core):
            n = LOW_CUT[core][1] if k in ("o", "d") else WIDTH[k]
            return send(swap[k].at[0, :, pl.ds(0, n)], swap[k].at[1, :, pl.ds(0, n)], sem, firsts[k].n, p.partner)

        def put(some):
            for u in some:
                swap[u.name][0, :, pl.ds(*u.span)] = u.total()

        put(units)
        for k in self.names:
            if k not in ("o", "d"):
                change(k, 0).start()
        for core in CORES:

            @pl.when(p.core == core)
            def _():
                put(low[core])
                for u in low[core]:
                    change(u.name, core).start()
                for k in self.names:
                    change(k, core).wait_send()
                    change(k, 1 - core).wait_recv()
                    half = ROWS[k] // 2
                    rows = pl.ds(core * half, half)
                    at = 0
                    for i in CORES:
                        n = LOW_CUT[i][1] if k in ("o", "d") else WIDTH[k]
                        part = swap[k][int(i != core), rows, pl.ds(0, n)]
                        if k in KEPT:
                            outs[k][i][...] = part
                        else:
                            outs[k][0][:, pl.ds(at, n)] = part
                        at += n
                for u in low[core]:
                    u.end()
        for u in units:
            u.end()

    def results(self, outs):
        outs = list(outs)
        return {k: [outs.pop(0) for _ in KEPT.get(k, [D])] for k in self.names}


def solution(mesh):
    cos, sin = rope_tables()

    def step(x, dy, *weights):
        w, mid, h, kept = forward(x[0], prep(*weights), cos, sin, 1)
        ids = iter(range(2, 100))
        by, grads, last = dy[0], [{}, {}], None
        for n in (1, 0):
            q, k, v, o, lse = kept[n]
            if n == 1:
                bymid, byo, delta, ggu, gd, go = after_back(by, h, o, w[n], fresh=True)
            else:
                (bymid, byo, delta, ggu, gd, go), more = after_back(by, mid, o, w[n], (ScatterJob(last), next(ids)))
                grads[1].update(more)
            big = dict(gu=ggu, d=gd) if n == 1 else dict(gu=ggu, d=gd, o=go)
            (dq, dk, dv), more = attend_back(q, k, v, byo, lse, delta, (ScatterJob(big), next(ids)))
            grads[n].update(more)
            by, gq, gkv = qkv_back(dq, dk, dv, h if n else x[0], bymid, w[n], cos, sin)
            last = dict(q=gq, kv=gkv, o=go) if n == 1 else dict(q=gq, kv=gkv)
        _, more = call(nothing, 1, [], [], link=(ScatterJob(last), next(ids)))
        grads[0].update(more)
        return (by[None], *(jnp.stack([g[k][i] for g in grads]) for k, i in (("q", 0), ("kv", 0), ("kv", 1), ("o", 0), ("gu", 0), ("gu", 1), ("d", 0))))

    states, cut = P(("rep", "dp"), None, None), P(None, "dp", None)
    return jax.shard_map(step, mesh=mesh, in_specs=(states, states) + (cut,) * 7, out_specs=(states,) + (P("rep", "dp", None),) * 7, check_vma=False)
```
